32 devices in a mesh: wide: 16 (over z, y, core), narrow: 2 (over x).
Axes of the slice: x: 2, y: 2, z: 4, core: 2. Of those that a mesh axis runs over, the one named last changes fastest.
Arguments:
- src_field: bfloat16 [2, 16, 65536], P(None, 'narrow', 'wide'), may hold values from -6 to 6
- src_depth: int32 [65536], P(('wide', 'narrow')), may hold values from 0 to 16, as said below
- packed_counts: int32 [4096, 64, 128], P(('wide', 'narrow')), may hold values from 0 to 100664832, as said below
- pair_source: int32 [4096], P(('wide', 'narrow')), may hold values from 0 to 15
- pair_home: int32 [4096], P(('wide', 'narrow')), may hold values from 0 to 1023, as said below
- pair_count: int32 [32], P(('wide', 'narrow')), may hold values from 64 to 128, as said below
Outputs:
- remapped: bfloat16 [2, 16, 131072], P(None, 'narrow', 'wide')
The draws below stay inside these ranges and needn't reach their ends.
Inputs may be any that keep to these rules, and one draw needn't show every extreme that they name: `src_depth`: depth 0 marks a dry source cell. `packed_counts`: word (p, i, j) holds count (p, i, j) plus 65536 times count (p, i + 64, j); every count lies between 0 and 1536. The target block pair_home[p] is held by wide index pair_home[p] // 64, which differs by at most 2, counted cyclically over the wide axis, from the wide index of the device that holds pair p. Among the 128 pairs of one device at most 51 have target blocks on one wide index, and on some wide index exactly 51 live pairs of that device. A device's pairs from position pair_count[d] on are padding; some device has all 128 live.
All inputs are finite; a program needn't handle non-finite values.
Results may differ from the reference program's by a relative error of at most 0.0054.
Values may be sent and summed in bfloat16 or wider, within the bound.
A program may use at most 64 MiB of HBM per device.

```python
import jax
import jax.numpy as jnp
from jax import lax

BLK = 128
LEV = 16
VARS = 2
DENOM = 256
REACH = 2
SB_DEV = 16
P_DEV = 128
TB_DEV = 64
CAP = 51
PAIRS = 4096
SRC_CELLS = 65536
N_WIDE = 16
N_NARROW = 2


def draw_src_depth(key, part):
    key = jax.random.fold_in(key, 404)
    key_land, key_depth = jax.random.split(key)
    blocks = SB_DEV * N_WIDE * N_NARROW
    sea_mask = (jax.random.randint(key_land, (blocks, 1), 0, 5) >= 3).astype(jnp.int32)
    cell_depth = jax.random.randint(key_depth, (blocks, BLK), 1, LEV + 1)
    return (cell_depth * sea_mask).reshape(blocks * BLK).astype(jnp.int32)


def draw_packed_counts(key, part):
    key = jax.random.fold_in(key, 101)
    half_rows = BLK // 2
    key_list = jax.random.split(key, 6)
    array_shape = (P_DEV * N_WIDE * N_NARROW, half_rows, BLK)
    row_ids = jnp.arange(half_rows, dtype=jnp.int32)[:, None]
    column_ids = jnp.arange(BLK, dtype=jnp.int32)[None, :]

    def half_counts(key_spread, key_power, key_factor, offset):
        spread = jax.random.randint(key_spread, array_shape, 0, 4)
        exponent = jax.random.randint(key_power, (array_shape[0], half_rows, 1), 0, 10)
        factor = jax.random.randint(key_factor, (array_shape[0], half_rows, 1), 1, 4)
        diagonal = jnp.power(2, exponent) * factor
        on_diagonal = (column_ids == row_ids + offset)[None, :, :]
        return jnp.where(on_diagonal, diagonal, spread)
    lower_half = half_counts(key_list[0], key_list[1], key_list[2], 0)
    upper_half = half_counts(key_list[3], key_list[4], key_list[5], half_rows)
    return (lower_half + 65536 * upper_half).astype(jnp.int32)


def draw_pair_home(key, part):
    key = jax.random.fold_in(key, 202)
    devices = N_WIDE * N_NARROW
    offset_total = 2 * REACH + 1
    key_rows, key_place = jax.random.split(key)
    head_rows = P_DEV // 2
    slot_ids = jnp.arange(offset_total * CAP, dtype=jnp.int32) // CAP
    wide_of = jnp.arange(devices, dtype=jnp.int32) // N_NARROW

    def one_device(row_key, wide_index):
        key_order, key_head, key_tail = jax.random.split(row_key, 3)
        offset_order = jax.random.permutation(key_order, offset_total).astype(jnp.int32)
        wanted = offset_order[slot_ids][:P_DEV]
        ordering = jnp.concatenate([jax.random.permutation(key_head, head_rows), head_rows + jax.random.permutation(key_tail, P_DEV - head_rows)])
        chosen = wanted[ordering]
        return (wide_index + chosen - REACH + N_WIDE) % N_WIDE
    owners = jax.vmap(one_device)(jax.random.split(key_rows, devices), wide_of)
    local_block = jax.random.randint(key_place, (devices, P_DEV), 0, TB_DEV)
    return (owners * TB_DEV + local_block).reshape(devices * P_DEV).astype(jnp.int32)


def draw_pair_count(key, part):
    key = jax.random.fold_in(key, 303)
    devices = N_WIDE * N_NARROW
    key_counts, key_full = jax.random.split(key)
    counts = jax.random.randint(key_counts, (devices,), P_DEV // 2, P_DEV + 1)
    fullest = jax.random.randint(key_full, (), 0, devices)
    return counts.at[fullest].set(P_DEV).astype(jnp.int32)


def with_ends(result, stream_key, low, high):
    dims = result.shape
    place = [jax.random.randint(jax.random.fold_in(stream_key, axis), (), 0, dims[axis]) for axis in range(len(dims))]
    result = result.at[tuple(place)].set(low)
    longest = dims.index(max(dims))
    place[longest] = (place[longest] + 1) % dims[longest]
    return result.at[tuple(place)].set(high)


def shard_levels(key, extent, cuts, smallest, high):
    def one(position, blocks):
        heights = jax.random.uniform(jax.random.fold_in(jax.random.fold_in(key, 6), position), (blocks,), jnp.float32, smallest / len(cuts), high / len(cuts))
        return jnp.repeat(jnp.exp(heights), extent[position] // blocks).reshape((-1,) + (1,) * (len(extent) - position - 1))

    loudness = one(*cuts[0])
    for cut in cuts[1:]:
        loudness = loudness * one(*cut)
    return loudness


def noise(stream_key, dims, width, most, cuts=(), kind=jnp.bfloat16):
    level = shard_levels(stream_key, dims, cuts, -0.22, 0.18) if cuts else 1.0
    drawn = jax.random.normal(stream_key, dims, jnp.float32) * width * level
    return jnp.minimum(jnp.maximum(drawn, -most), most).astype(kind)


def setup_inputs(seed: int = 0) -> dict:
    streams_of = jax.random.split(jax.random.key(seed), 7)
    src_field = noise(streams_of[0], (VARS, LEV, SRC_CELLS), 1.0, 6.0, ((1, 2), (2, 16)))
    src_depth = draw_src_depth(jax.random.fold_in(streams_of[6], 71), 0)
    packed_counts = draw_packed_counts(jax.random.fold_in(streams_of[6], 71), 0)
    pair_source = with_ends(jax.random.randint(streams_of[3], (PAIRS,), 0, SB_DEV), jax.random.fold_in(streams_of[3], 1), 0, SB_DEV - 1).astype(jnp.int32)
    pair_home = draw_pair_home(jax.random.fold_in(streams_of[6], 71), 0)
    pair_count = draw_pair_count(jax.random.fold_in(streams_of[6], 71), 0)
    return dict(src_field=src_field, src_depth=src_depth, packed_counts=packed_counts, pair_source=pair_source, pair_home=pair_home, pair_count=pair_count)


wet_limit = 1e-3


def unpack_counts(packed_words):
    lower_half = packed_words % 65536
    upper_half = packed_words // 65536
    return jnp.concatenate([lower_half, upper_half], axis=-2)


def stack_cells(field_block, depth_cells):
    level_ids = jnp.arange(field_block.shape[1], dtype=jnp.int32)
    wet_levels = level_ids[:, None] < depth_cells[None, :]
    masked = jnp.where(wet_levels[None, :, :], field_block, jnp.zeros_like(field_block))
    wet_ones = wet_levels.astype(field_block.dtype)
    return jnp.concatenate([jnp.transpose(masked, (1, 0, 2)), wet_ones[:, None, :]], axis=1)


def reference(src_field, src_depth, packed_counts, pair_source, pair_home, pair_count):
    device_total = pair_count.shape[0]
    own_cells = SB_DEV * BLK
    components = VARS + 1
    block_total = jnp.zeros((TB_DEV * N_WIDE, LEV, components, BLK), jnp.float32)

    def add_device(device_index, running):
        device_index = device_index.astype(jnp.int32)
        device_field = lax.dynamic_slice_in_dim(src_field, device_index * own_cells, own_cells, 2)
        cell_depth = lax.dynamic_slice_in_dim(src_depth, device_index * own_cells, own_cells, 0)
        device_packed = lax.dynamic_slice_in_dim(packed_counts, device_index * P_DEV, P_DEV, 0)
        source = lax.dynamic_slice_in_dim(pair_source, device_index * P_DEV, P_DEV, 0)
        home_block = lax.dynamic_slice_in_dim(pair_home, device_index * P_DEV, P_DEV, 0)
        live_count = lax.dynamic_slice_in_dim(pair_count, device_index, 1, 0)[0]
        stacked = stack_cells(device_field, cell_depth).reshape(LEV, components, SB_DEV, BLK)
        picked = jnp.take(stacked, source, axis=2)
        weight = (unpack_counts(device_packed).astype(jnp.float32) / DENOM).astype(jnp.bfloat16)
        pair_terms = jnp.einsum("pts,lcps->plct", weight.astype(jnp.float32), picked.astype(jnp.float32))
        pair_terms = lax.optimization_barrier(pair_terms.astype(jnp.bfloat16)).astype(jnp.float32)
        is_live = jnp.arange(P_DEV, dtype=jnp.int32) < live_count
        pair_terms = jnp.where(is_live[:, None, None, None], pair_terms, jnp.zeros_like(pair_terms))
        return running.at[home_block].add(pair_terms)

    block_total = lax.fori_loop(0, device_total, add_device, block_total)
    numerators = block_total[:, :, :VARS, :]
    wet_total = block_total[:, :, VARS, :]
    covered = wet_total > wet_limit
    safe_wet = jnp.where(covered, wet_total, jnp.ones_like(wet_total))
    remapped = jnp.where(covered[:, :, None, :], numerators / safe_wet[:, :, None, :], jnp.zeros_like(numerators))
    remapped = jnp.transpose(remapped, (2, 1, 0, 3)).reshape(VARS, LEV, TB_DEV * N_WIDE * BLK)
    return remapped.astype(jnp.bfloat16)
```

```python
import functools

import jax
import jax.numpy as jnp
from jax import lax
from jax.experimental import pallas as pl
from jax.experimental.pallas import tpu as pltpu
from jax.sharding import PartitionSpec as P

DENOM = 256
REACH = 2
TB_DEV = 64


wet_limit = 0.001


def passed_along(block, axis, distance):
    devices = range(lax.axis_size(axis))
    route = [((i - distance) % len(devices), i) for i in devices]
    return lax.ppermute(block, axis, route)


def unpack_counts(packed_words):
    return jnp.concatenate([packed_words % 65536, packed_words // 65536], axis=-2)


def block_sums(targets, received, block_count):
    owners = jnp.arange(block_count, dtype=jnp.int32)
    select = (targets[:, None] == owners[None, :]).astype(jnp.bfloat16)
    return jnp.einsum("rq,rlcb->lcqb", select, received, preferred_element_type=jnp.float32)


def by_collectives(src_field, src_depth, packed_counts, pair_source, pair_home, pair_count):
    narrow_size = lax.axis_size("narrow")
    wide_size = lax.axis_size("wide")
    field_vars = src_field.shape[0]
    components = field_vars + 1
    block_cells = packed_counts.shape[2]
    own_cells = src_depth.shape[0]
    own_tiles = own_cells // block_cells
    pair_slots = pair_source.shape[0]
    offset_count = 2 * REACH + 1
    capacity = max(2, 2 * pair_slots // offset_count)
    own_field = lax.all_to_all(src_field, "narrow", split_axis=2, concat_axis=1, tiled=True)
    levels = own_field.shape[1]
    part_levels = levels // narrow_size
    level_ids = jnp.arange(levels, dtype=jnp.int32)
    wet_levels = level_ids[:, None] < src_depth[None, :]
    masked = jnp.where(wet_levels[None, :, :], own_field, jnp.zeros_like(own_field))
    stacked = jnp.concatenate(
        [jnp.transpose(masked, (1, 0, 2)), wet_levels.astype(jnp.bfloat16)[:, None, :]], axis=1
    )
    by_tile = jnp.transpose(stacked.reshape(levels * components, own_tiles, block_cells), (1, 0, 2))
    picked = jnp.take(by_tile, pair_source, axis=0)
    weight = (unpack_counts(packed_counts).astype(jnp.float32) / DENOM).astype(jnp.bfloat16)
    pair_terms = lax.dot_general(
        picked, weight, (((2,), (2,)), ((0,), (0,))), preferred_element_type=jnp.float32
    )
    pair_terms = pair_terms.astype(jnp.bfloat16)
    is_live = jnp.arange(pair_slots, dtype=jnp.int32) < pair_count[0]
    wide_index = lax.axis_index("wide")
    destination = pair_home // TB_DEV
    local_block = pair_home % TB_DEV
    offset_index = (destination - wide_index + REACH + wide_size) % wide_size
    bound_for = (
        (offset_index[:, None] == jnp.arange(offset_count, dtype=jnp.int32)[None, :])
        & is_live[:, None]
    ).astype(jnp.int32)
    before = jnp.cumsum(bound_for, axis=0) - bound_for
    position = jnp.sum(before * bound_for, axis=1)
    slot_index = jnp.where(is_live, offset_index * capacity + position, offset_count * capacity)
    outgoing = (
        jnp.zeros((offset_count * capacity, levels * components, block_cells), jnp.bfloat16)
        .at[slot_index]
        .set(pair_terms, mode="drop")
    )
    targets = (
        jnp.full((offset_count * capacity,), TB_DEV, jnp.int32)
        .at[slot_index]
        .set(local_block, mode="drop")
    )
    outgoing = outgoing.reshape(offset_count, capacity, levels, components, block_cells)
    targets = targets.reshape(offset_count, capacity)
    shift_list = [shift_by for shift_by in range(-REACH, REACH + 1) if shift_by != 0]
    partial_value = block_sums(targets[REACH], outgoing[REACH], TB_DEV)
    for shift_by in shift_list:
        moved_terms, moved_owners = passed_along(
            (outgoing[REACH + shift_by], targets[REACH + shift_by]), "wide", shift_by
        )
        partial_value = partial_value + block_sums(moved_owners, moved_terms, TB_DEV)
    block_totals = lax.psum_scatter(partial_value, "narrow", scatter_dimension=0, tiled=True)
    numerators = block_totals[:, :field_vars]
    wet_total = block_totals[:, field_vars]
    covered = wet_total > wet_limit
    safe_wet = jnp.where(covered, wet_total, jnp.ones_like(wet_total))
    result = jnp.where(covered[:, None], numerators / safe_wet[:, None], jnp.zeros_like(numerators))
    result = jnp.transpose(result, (1, 0, 2, 3)).reshape(
        field_vars, part_levels, TB_DEV * block_cells
    )
    return result.astype(jnp.bfloat16)


SELF, MATE, RELAY, AHEAD, BEHIND = range(5)
PARTS = 4
LOADS = 8
UNROLL = 4


def remap_kernel(
    sizes,
    field_ref,
    depth_ref,
    source_ref,
    home_ref,
    packed_ref,
    out_ref,
    field_in,
    home_in,
    words,
    weight,
    stacked,
    terms,
    cross_out,
    cross_in,
    own_terms,
    self_sum,
    sums_out,
    mate_in,
    ahead_in,
    behind_in,
    load_sems,
    entry_sems,
    cross_sems,
    mate_sems,
    ahead_sems,
    behind_sems,
):
    wide_size, fields, levels, tiles, cells, pairs = sizes
    rows = (fields + 1) * levels
    part_levels = levels // PARTS
    part_rows = rows // PARTS
    w = lax.axis_index("wide")
    n = lax.axis_index("narrow")
    other = 1 - n
    sign = 1 - 2 * lax.rem(w, 2)
    mate = w + sign
    ahead = lax.rem(w + 2 * sign + wide_size, wide_size)
    behind = lax.rem(w - 2 * sign + wide_size, wide_size)

    per_load = pairs // LOADS
    loads = []
    for i in range(LOADS):
        span = pl.ds(i * per_load, per_load)
        load = pltpu.make_async_copy(packed_ref.at[span], words.at[span], load_sems.at[i])
        load.start()
        loads.append(load)

    def remote(src, dst, sems, index, place):
        return pltpu.make_async_remote_copy(
            src_ref=src,
            dst_ref=dst,
            send_sem=sems.at[0, index],
            recv_sem=sems.at[1, index],
            device_id=place,
            device_id_type=pl.DeviceIdType.MESH,
        )

    barrier = pltpu.get_barrier_semaphore()
    for place in ((w, other), (mate, n), (ahead, n), (behind, n)):
        pl.semaphore_signal(
            barrier, inc=1, device_id=place, device_id_type=pl.DeviceIdType.MESH
        )
    pl.semaphore_wait(barrier, 4)

    own_cells = tiles * cells
    entry = [
        remote(
            field_ref.at[:, :, pl.ds(pl.multiple_of(other * own_cells, own_cells), own_cells)],
            field_in,
            entry_sems,
            0,
            (w, other),
        ),
        remote(home_ref, home_in, entry_sems, 1, (w, other)),
    ]
    for copy in entry:
        copy.start()

    level_ids = lax.broadcasted_iota(jnp.int32, (levels, cells), 0)

    def stack(side, group, read):
        for tile in range(tiles):
            wet = level_ids + group * levels < depth_ref[pl.ds(tile, 1), :]
            for k in range(fields):
                value = read(k, tile).astype(jnp.float32)
                stacked[side * tiles + tile, pl.ds(k * levels, levels), :] = jnp.where(
                    wet, value, 0.0
                )
            stacked[side * tiles + tile, pl.ds(fields * levels, levels), :] = jnp.where(
                wet, 1.0, 0.0
            )

    own_start = n * own_cells
    stack(
        0,
        n,
        lambda k, tile: field_ref[
            k, :, pl.ds(pl.multiple_of(own_start + tile * cells, cells), cells)
        ],
    )

    half = cells // 2
    for i in range(LOADS):
        loads[i].wait()

        def unpack(step, carry):
            for u in range(UNROLL):
                p = i * per_load + step * UNROLL + u
                word = words[p]
                low = (word & 65535).astype(jnp.float32).astype(jnp.bfloat16)
                high = (word >> 16).astype(jnp.float32).astype(jnp.bfloat16)
                weight[p, pl.ds(0, half), :] = low
                weight[p, pl.ds(half, half), :] = high
            return carry

        lax.fori_loop(0, per_load // UNROLL, unpack, 0)

    entry[0].wait()
    stack(1, other, lambda k, tile: field_in[k, :, pl.ds(tile * cells, cells)])

    def multiply(side):
        def body(step, carry):
            for u in range(UNROLL):
                p = step * UNROLL + u
                values = stacked[side * tiles + source_ref[p]].astype(jnp.bfloat16)
                term = lax.dot_general(
                    values, weight[p], (((1,), (1,)), ((), ())),
                    preferred_element_type=jnp.float32,
                )
                terms[pl.ds(p, rows, stride=pairs), :] = term * (1.0 / DENOM)
            return carry

        lax.fori_loop(0, pairs // UNROLL, body, 0)

    def rounded(part, row):
        k, level = row // part_levels, part * part_levels + row % part_levels
        return terms[pl.ds((k * levels + level) * pairs, pairs), :].astype(jnp.bfloat16)

    multiply(1)
    cross = []
    for part in range(PARTS):
        for row in range(part_rows):
            cross_out[part, row] = rounded(part, row)
        copy = remote(cross_out.at[part], cross_in.at[part], cross_sems, part, (w, other))
        copy.start()
        cross.append(copy)

    multiply(0)
    for part in range(PARTS):
        for row in range(part_rows):
            own_terms[part, row] = rounded(part, row)

    entry[1].wait()
    slots = lax.broadcasted_iota(jnp.int32, (5 * TB_DEV, pairs), 0)
    select = jnp.concatenate(
        [
            jnp.where(slots == home_ref[...], 1.0, 0.0).astype(jnp.bfloat16),
            jnp.where(slots == home_in[...], 1.0, 0.0).astype(jnp.bfloat16),
        ],
        axis=1,
    )

    to_mate, to_ahead, to_behind = [], [], []

    def pass_on(part):
        to_mate[part].wait_recv()
        for row in range(part_rows):
            sums_out[part, AHEAD - 1, row] = (
                sums_out[part, AHEAD - 1, row].astype(jnp.float32)
                + mate_in[part, RELAY - 1, row].astype(jnp.float32)
            ).astype(jnp.bfloat16)
        copy = remote(
            sums_out.at[part, AHEAD - 1], ahead_in.at[part], ahead_sems, part, (ahead, n)
        )
        copy.start()
        to_ahead.append(copy)

    for part in range(PARTS):
        cross[part].wait_recv()
        for row in range(part_rows):
            pair_values = jnp.concatenate([own_terms[part, row], cross_in[part, row]], axis=0)
            sums = jnp.dot(select, pair_values, preferred_element_type=jnp.float32)
            self_sum[part, row] = sums[:TB_DEV]
            for slot in (MATE, RELAY, AHEAD, BEHIND):
                sums_out[part, slot - 1, row] = sums[
                    slot * TB_DEV : (slot + 1) * TB_DEV
                ].astype(jnp.bfloat16)
        copy = remote(
            sums_out.at[part, pl.ds(0, 2)], mate_in.at[part], mate_sems, part, (mate, n)
        )
        copy.start()
        to_mate.append(copy)
        copy = remote(
            sums_out.at[part, BEHIND - 1], behind_in.at[part], behind_sems, part, (behind, n)
        )
        copy.start()
        to_behind.append(copy)
        if part > 0:
            pass_on(part - 1)
    pass_on(PARTS - 1)

    for part in range(PARTS):
        to_behind[part].wait_recv()
        to_ahead[part].wait_recv()

        def total(row):
            return (
                self_sum[part, row]
                + mate_in[part, MATE - 1, row].astype(jnp.float32)
                + ahead_in[part, row].astype(jnp.float32)
                + behind_in[part, row].astype(jnp.float32)
            )

        for j in range(part_levels):
            wet_total = total(fields * part_levels + j)
            covered = wet_total > wet_limit
            safe_wet = jnp.where(covered, wet_total, 1.0)
            for k in range(fields):
                ratio = total(k * part_levels + j) / safe_wet
                out_ref[k, part * part_levels + j] = jnp.where(covered, ratio, 0.0).astype(
                    out_ref.dtype
                )
    for part in range(PARTS):
        cross[part].wait_send()
        to_mate[part].wait_send()
        to_ahead[part].wait_send()
        to_behind[part].wait_send()


def by_kernel(src_field, src_depth, packed_counts, pair_source, pair_home, pair_count):
    wide_size = lax.axis_size("wide")
    fields, levels, _ = src_field.shape
    pairs, _, cells = packed_counts.shape
    tiles = src_depth.shape[0] // cells
    rows = (fields + 1) * levels
    part_rows = rows // PARTS
    wide_index = lax.axis_index("wide")
    sign = 1 - 2 * (wide_index % 2)
    offset = (pair_home // TB_DEV - wide_index + REACH + wide_size) % wide_size - REACH
    toward = offset * sign
    slot = jnp.where(toward > 0, 2 * toward - 1, -2 * toward)
    is_live = jnp.arange(pairs, dtype=jnp.int32) < pair_count[0]
    home = jnp.where(is_live, slot * TB_DEV + pair_home % TB_DEV, -1)
    sizes = (wide_size, fields, levels, tiles, cells, pairs)
    vmem = pl.BlockSpec(memory_space=pltpu.VMEM)
    bf16, f32, i32 = jnp.bfloat16, jnp.float32, jnp.int32
    sums_shape = (PARTS, part_rows, TB_DEV, cells)
    copies = pltpu.SemaphoreType.DMA((2, PARTS))
    result = pl.pallas_call(
        functools.partial(remap_kernel, sizes),
        out_shape=jax.ShapeDtypeStruct((fields, levels, TB_DEV, cells), bf16),
        in_specs=[
            vmem,
            vmem,
            pl.BlockSpec(memory_space=pltpu.SMEM),
            vmem,
            pl.BlockSpec(memory_space=pl.ANY),
        ],
        out_specs=vmem,
        scratch_shapes=[
            pltpu.VMEM((fields, levels, tiles * cells), bf16),
            pltpu.VMEM((1, pairs), i32),
            pltpu.VMEM((pairs, cells // 2, cells), i32),
            pltpu.VMEM((pairs, cells, cells), bf16),
            pltpu.VMEM((2 * tiles, rows, cells), f32),
            pltpu.VMEM((rows * pairs, cells), f32),
            pltpu.VMEM((PARTS, part_rows, pairs, cells), bf16),
            pltpu.VMEM((PARTS, part_rows, pairs, cells), bf16),
            pltpu.VMEM((PARTS, part_rows, pairs, cells), bf16),
            pltpu.VMEM(sums_shape, f32),
            pltpu.VMEM((PARTS, 4) + sums_shape[1:], bf16),
            pltpu.VMEM((PARTS, 2) + sums_shape[1:], bf16),
            pltpu.VMEM(sums_shape, bf16),
            pltpu.VMEM(sums_shape, bf16),
            pltpu.SemaphoreType.DMA((LOADS,)),
            pltpu.SemaphoreType.DMA((2, 2)),
            copies,
            copies,
            copies,
            copies,
        ],
        compiler_params=pltpu.CompilerParams(
            collective_id=0, has_side_effects=True, vmem_limit_bytes=48 * 1024 * 1024
        ),
        name="remap",
    )(
        src_field,
        src_depth.reshape(tiles, cells),
        pair_source,
        home.reshape(1, pairs),
        packed_counts,
    )
    return result.reshape(fields, levels, TB_DEV * cells)


def solution(mesh):
    placed = (
        P(None, "narrow", "wide"),
        P(("wide", "narrow")),
        P(("wide", "narrow"), None, None),
        P(("wide", "narrow")),
        P(("wide", "narrow")),
        P(("wide", "narrow")),
    )
    paired = mesh.shape["narrow"] == 2 and mesh.shape["wide"] % 2 == 0
    fits = paired and mesh.shape["wide"] > 2 * REACH and REACH == 2
    return jax.shard_map(
        by_kernel if fits else by_collectives,
        mesh=mesh,
        in_specs=placed,
        out_specs=P(None, "narrow", "wide"),
        check_vma=False,
    )
```

```python
import functools

import jax
import jax.numpy as jnp
from jax import lax
from jax.experimental import pallas as pl
from jax.experimental.pallas import tpu as pltpu
from jax.sharding import PartitionSpec as P

DENOM = 256
REACH = 2
TB_DEV = 64


wet_limit = 0.001


def passed_along(block, axis, distance):
    devices = range(lax.axis_size(axis))
    route = [((i - distance) % len(devices), i) for i in devices]
    return lax.ppermute(block, axis, route)


def unpack_counts(packed_words):
    return jnp.concatenate([packed_words % 65536, packed_words // 65536], axis=-2)


def block_sums(targets, received, block_count):
    owners = jnp.arange(block_count, dtype=jnp.int32)
    select = (targets[:, None] == owners[None, :]).astype(jnp.bfloat16)
    return jnp.einsum("rq,rlcb->lcqb", select, received, preferred_element_type=jnp.float32)


def by_collectives(src_field, src_depth, packed_counts, pair_source, pair_home, pair_count):
    narrow_size = lax.axis_size("narrow")
    wide_size = lax.axis_size("wide")
    field_vars = src_field.shape[0]
    components = field_vars + 1
    block_cells = packed_counts.shape[2]
    own_cells = src_depth.shape[0]
    own_tiles = own_cells // block_cells
    pair_slots = pair_source.shape[0]
    offset_count = 2 * REACH + 1
    capacity = max(2, 2 * pair_slots // offset_count)
    own_field = lax.all_to_all(src_field, "narrow", split_axis=2, concat_axis=1, tiled=True)
    levels = own_field.shape[1]
    part_levels = levels // narrow_size
    level_ids = jnp.arange(levels, dtype=jnp.int32)
    wet_levels = level_ids[:, None] < src_depth[None, :]
    masked = jnp.where(wet_levels[None, :, :], own_field, jnp.zeros_like(own_field))
    stacked = jnp.concatenate(
        [jnp.transpose(masked, (1, 0, 2)), wet_levels.astype(jnp.bfloat16)[:, None, :]], axis=1
    )
    by_tile = jnp.transpose(stacked.reshape(levels * components, own_tiles, block_cells), (1, 0, 2))
    picked = jnp.take(by_tile, pair_source, axis=0)
    weight = (unpack_counts(packed_counts).astype(jnp.float32) / DENOM).astype(jnp.bfloat16)
    pair_terms = lax.dot_general(
        picked, weight, (((2,), (2,)), ((0,), (0,))), preferred_element_type=jnp.float32
    )
    pair_terms = pair_terms.astype(jnp.bfloat16)
    is_live = jnp.arange(pair_slots, dtype=jnp.int32) < pair_count[0]
    wide_index = lax.axis_index("wide")
    destination = pair_home // TB_DEV
    local_block = pair_home % TB_DEV
    offset_index = (destination - wide_index + REACH + wide_size) % wide_size
    bound_for = (
        (offset_index[:, None] == jnp.arange(offset_count, dtype=jnp.int32)[None, :])
        & is_live[:, None]
    ).astype(jnp.int32)
    before = jnp.cumsum(bound_for, axis=0) - bound_for
    position = jnp.sum(before * bound_for, axis=1)
    slot_index = jnp.where(is_live, offset_index * capacity + position, offset_count * capacity)
    outgoing = (
        jnp.zeros((offset_count * capacity, levels * components, block_cells), jnp.bfloat16)
        .at[slot_index]
        .set(pair_terms, mode="drop")
    )
    targets = (
        jnp.full((offset_count * capacity,), TB_DEV, jnp.int32)
        .at[slot_index]
        .set(local_block, mode="drop")
    )
    outgoing = outgoing.reshape(offset_count, capacity, levels, components, block_cells)
    targets = targets.reshape(offset_count, capacity)
    shift_list = [shift_by for shift_by in range(-REACH, REACH + 1) if shift_by != 0]
    partial_value = block_sums(targets[REACH], outgoing[REACH], TB_DEV)
    for shift_by in shift_list:
        moved_terms, moved_owners = passed_along(
            (outgoing[REACH + shift_by], targets[REACH + shift_by]), "wide", shift_by
        )
        partial_value = partial_value + block_sums(moved_owners, moved_terms, TB_DEV)
    block_totals = lax.psum_scatter(partial_value, "narrow", scatter_dimension=0, tiled=True)
    numerators = block_totals[:, :field_vars]
    wet_total = block_totals[:, field_vars]
    covered = wet_total > wet_limit
    safe_wet = jnp.where(covered, wet_total, jnp.ones_like(wet_total))
    result = jnp.where(covered[:, None], numerators / safe_wet[:, None], jnp.zeros_like(numerators))
    result = jnp.transpose(result, (1, 0, 2, 3)).reshape(
        field_vars, part_levels, TB_DEV * block_cells
    )
    return result.astype(jnp.bfloat16)


SELF, MATE, RELAY, AHEAD, BEHIND = range(5)
LOADS = 8
BATCHES = 4
EARLY = 3
UNROLL = 4


def remap_kernel(
    sizes,
    field_hbm,
    depth_hbm,
    packed_hbm,
    source_hbm,
    home_hbm,
    count_hbm,
    out_ref,
    field,
    depth,
    source,
    home,
    count,
    field_in,
    slot_own,
    slot_in,
    words,
    weight,
    stacked,
    terms,
    cross_out,
    cross_in,
    own_terms,
    self_sum,
    sums_out,
    mate_in,
    ahead_in,
    behind_in,
    load_sems,
    small_sems,
    entry_sems,
    early_sems,
    cross_sems,
    mate_sems,
    ahead_sems,
    behind_sems,
):
    wide_size, fields, levels, tiles, cells, pairs = sizes
    components = fields + 1
    rows = components * levels
    w = lax.axis_index("wide")
    n = lax.axis_index("narrow")
    other = 1 - n
    sign = 1 - 2 * lax.rem(w, 2)
    mate = w + sign
    ahead = lax.rem(w + 2 * sign + wide_size, wide_size)
    behind = lax.rem(w - 2 * sign + wide_size, wide_size)

    barrier = pltpu.get_barrier_semaphore()
    for place in ((w, other), (mate, n), (ahead, n), (behind, n)):
        pl.semaphore_signal(
            barrier, inc=1, device_id=place, device_id_type=pl.DeviceIdType.MESH
        )

    small = []
    for i, (src, dst) in enumerate(
        (
            (field_hbm, field),
            (home_hbm, home),
            (count_hbm, count),
            (depth_hbm, depth),
            (source_hbm, source),
        )
    ):
        load = pltpu.make_async_copy(src, dst, small_sems.at[i])
        load.start()
        small.append(load)
    per_load = pairs // LOADS
    loads = []
    for i in range(LOADS):
        span = pl.ds(i * per_load, per_load)
        load = pltpu.make_async_copy(packed_hbm.at[span], words.at[span], load_sems.at[i])
        load.start()
        loads.append(load)

    def remote(src, dst, sems, index, place):
        return pltpu.make_async_remote_copy(
            src_ref=src,
            dst_ref=dst,
            send_sem=sems.at[(0,) + index],
            recv_sem=sems.at[(1,) + index],
            device_id=place,
            device_id_type=pl.DeviceIdType.MESH,
        )

    small[0].wait()
    small[1].wait()
    small[2].wait()
    wide_home = lax.div(home[...], TB_DEV)
    offset = lax.rem(wide_home - w + REACH + wide_size, wide_size) - REACH
    toward = offset * sign
    slot = jnp.where(toward > 0, 2 * toward - 1, -2 * toward)
    is_live = lax.broadcasted_iota(jnp.int32, (1, pairs), 1) < count[0]
    slot_own[...] = jnp.where(is_live, slot * TB_DEV + home[...] - wide_home * TB_DEV, -1)

    pl.semaphore_wait(barrier, 4)
    own_cells = tiles * cells
    entry = [
        remote(
            field.at[:, :, pl.ds(pl.multiple_of(other * own_cells, own_cells), own_cells)],
            field_in,
            entry_sems,
            (0,),
            (w, other),
        ),
        remote(slot_own, slot_in, entry_sems, (1,), (w, other)),
    ]
    for copy in entry:
        copy.start()

    level_ids = lax.broadcasted_iota(jnp.int32, (levels, cells), 0)

    def stack(side, group, read):
        for tile in range(tiles):
            wet = level_ids + group * levels < depth[pl.ds(tile, 1), :]
            for k in range(components):
                value = read(k, tile).astype(jnp.float32) if k < fields else 1.0
                stacked[tile, pl.ds(side * rows + k * levels, levels), :] = jnp.where(
                    wet, value, 0.0
                )

    small[3].wait()
    small[4].wait()
    own_start = n * own_cells
    stack(
        1,
        n,
        lambda k, tile: field[k, :, pl.ds(pl.multiple_of(own_start + tile * cells, cells), cells)],
    )

    half = cells // 2
    for i in range(LOADS):
        loads[i].wait()

        def unpack(step, carry):
            for u in range(UNROLL):
                p = i * per_load + step * UNROLL + u
                word = words[p]
                low = (word & 65535).astype(jnp.float32).astype(jnp.bfloat16)
                high = (word >> 16).astype(jnp.float32).astype(jnp.bfloat16)
                weight[p, pl.ds(0, half), :] = low
                weight[p, pl.ds(half, half), :] = high
            return carry

        lax.fori_loop(0, per_load // UNROLL, unpack, 0)

    entry[0].wait()
    stack(0, other, lambda k, tile: field_in[k, :, pl.ds(tile * cells, cells)])

    per_batch = pairs // BATCHES

    def rounded(side, level, k, start, count):
        row = side * rows + k * levels + level
        return terms[pl.ds(row * pairs + start, count), :].astype(jnp.bfloat16)

    cross = []
    for batch in range(BATCHES):
        first = batch * per_batch

        def multiply(step, carry):
            for u in range(UNROLL):
                p = first + step * UNROLL + u
                values = stacked[source[p]].astype(jnp.bfloat16)
                term = lax.dot_general(
                    values, weight[p], (((1,), (1,)), ((), ())),
                    preferred_element_type=jnp.float32,
                )
                terms[pl.ds(p, 2 * rows, stride=pairs), :] = term * (1.0 / DENOM)
            return carry

        lax.fori_loop(0, per_batch // UNROLL, multiply, 0)
        span = pl.ds(first, per_batch)
        for level in range(EARLY):
            for k in range(components):
                cross_out[level, k, span, :] = rounded(0, level, k, first, per_batch)
            copy = remote(
                cross_out.at[level, :, span, :],
                cross_in.at[level, :, span, :],
                early_sems,
                (level, batch),
                (w, other),
            )
            copy.start()
            cross.append((level, copy))
    for level in range(EARLY, levels):
        for k in range(components):
            cross_out[level, k] = rounded(0, level, k, 0, pairs)
        copy = remote(
            cross_out.at[level], cross_in.at[level], cross_sems, (level - EARLY,), (w, other)
        )
        copy.start()
        cross.append((level, copy))
    for level in range(levels):
        for k in range(components):
            own_terms[level, k] = rounded(1, level, k, 0, pairs)

    entry[1].wait()
    slots = lax.broadcasted_iota(jnp.int32, (5 * TB_DEV, pairs), 0)
    select = jnp.concatenate(
        [
            jnp.where(slots == slot_own[...], 1.0, 0.0).astype(jnp.bfloat16),
            jnp.where(slots == slot_in[...], 1.0, 0.0).astype(jnp.bfloat16),
        ],
        axis=1,
    )

    to_mate, to_ahead, to_behind = [], [], []

    def pass_on(level):
        to_mate[level].wait_recv()
        for k in range(components):
            sums_out[level, AHEAD - 1, k] = (
                sums_out[level, AHEAD - 1, k].astype(jnp.float32)
                + mate_in[level, RELAY - 1, k].astype(jnp.float32)
            ).astype(jnp.bfloat16)
        copy = remote(
            sums_out.at[level, AHEAD - 1], ahead_in.at[level], ahead_sems, (level,), (ahead, n)
        )
        copy.start()
        to_ahead.append(copy)

    for level in range(levels):
        for of_level, copy in cross:
            if of_level == level:
                copy.wait_recv()
        for k in range(components):
            pair_values = jnp.concatenate([own_terms[level, k], cross_in[level, k]], axis=0)
            sums = jnp.dot(select, pair_values, preferred_element_type=jnp.float32)
            self_sum[level, k] = sums[:TB_DEV]
            for slot in (MATE, RELAY, AHEAD, BEHIND):
                sums_out[level, slot - 1, k] = sums[
                    slot * TB_DEV : (slot + 1) * TB_DEV
                ].astype(jnp.bfloat16)
        copy = remote(
            sums_out.at[level, pl.ds(0, 2)], mate_in.at[level], mate_sems, (level,), (mate, n)
        )
        copy.start()
        to_mate.append(copy)
        copy = remote(
            sums_out.at[level, BEHIND - 1], behind_in.at[level], behind_sems, (level,), (behind, n)
        )
        copy.start()
        to_behind.append(copy)
        if level > 0:
            pass_on(level - 1)
    pass_on(levels - 1)

    for level in range(levels):
        to_behind[level].wait_recv()
        to_ahead[level].wait_recv()

        def total(k):
            return (
                self_sum[level, k]
                + mate_in[level, MATE - 1, k].astype(jnp.float32)
                + ahead_in[level, k].astype(jnp.float32)
                + behind_in[level, k].astype(jnp.float32)
            )

        wet_total = total(fields)
        covered = wet_total > wet_limit
        safe_wet = jnp.where(covered, wet_total, 1.0)
        for k in range(fields):
            out_ref[k, level] = jnp.where(covered, total(k) / safe_wet, 0.0).astype(out_ref.dtype)
    for _, copy in cross:
        copy.wait_send()
    for copy in to_mate + to_ahead + to_behind:
        copy.wait_send()


def by_kernel(src_field, src_depth, packed_counts, pair_source, pair_home, pair_count):
    wide_size = lax.axis_size("wide")
    fields, levels, _ = src_field.shape
    pairs, _, cells = packed_counts.shape
    tiles = src_depth.shape[0] // cells
    components = fields + 1
    rows = components * levels
    sizes = (wide_size, fields, levels, tiles, cells, pairs)
    hbm = pl.BlockSpec(memory_space=pltpu.HBM)
    bf16, f32, i32 = jnp.bfloat16, jnp.float32, jnp.int32
    terms_shape = (levels, components, pairs, cells)
    sums_shape = (components, TB_DEV, cells)
    copies = pltpu.SemaphoreType.DMA((2, levels))
    result = pl.pallas_call(
        functools.partial(remap_kernel, sizes),
        out_shape=jax.ShapeDtypeStruct((fields, levels, TB_DEV, cells), bf16),
        in_specs=[hbm] * 6,
        out_specs=pl.BlockSpec(memory_space=pltpu.VMEM),
        scratch_shapes=[
            pltpu.VMEM(src_field.shape, bf16),
            pltpu.VMEM((tiles, cells), i32),
            pltpu.SMEM((pairs,), i32),
            pltpu.VMEM((1, pairs), i32),
            pltpu.SMEM((1,), i32),
            pltpu.VMEM((fields, levels, tiles * cells), bf16),
            pltpu.VMEM((1, pairs), i32),
            pltpu.VMEM((1, pairs), i32),
            pltpu.VMEM((pairs, cells // 2, cells), i32),
            pltpu.VMEM((pairs, cells, cells), bf16),
            pltpu.VMEM((tiles, 2 * rows, cells), f32),
            pltpu.VMEM((2 * rows * pairs, cells), f32),
            pltpu.VMEM(terms_shape, bf16),
            pltpu.VMEM(terms_shape, bf16),
            pltpu.VMEM(terms_shape, bf16),
            pltpu.VMEM((levels,) + sums_shape, f32),
            pltpu.VMEM((levels, 4) + sums_shape, bf16),
            pltpu.VMEM((levels, 2) + sums_shape, bf16),
            pltpu.VMEM((levels,) + sums_shape, bf16),
            pltpu.VMEM((levels,) + sums_shape, bf16),
            pltpu.SemaphoreType.DMA((LOADS,)),
            pltpu.SemaphoreType.DMA((5,)),
            pltpu.SemaphoreType.DMA((2, 2)),
            pltpu.SemaphoreType.DMA((2, EARLY, BATCHES)),
            pltpu.SemaphoreType.DMA((2, levels - EARLY)),
            copies,
            copies,
            copies,
        ],
        compiler_params=pltpu.CompilerParams(
            collective_id=0, has_side_effects=True, vmem_limit_bytes=67043328
        ),
        name="remap",
    )(
        src_field,
        src_depth.reshape(tiles, cells),
        packed_counts,
        pair_source,
        pair_home.reshape(1, pairs),
        pair_count,
    )
    return result.reshape(fields, levels, TB_DEV * cells)


def solution(mesh):
    placed = (
        P(None, "narrow", "wide"),
        P(("wide", "narrow")),
        P(("wide", "narrow"), None, None),
        P(("wide", "narrow")),
        P(("wide", "narrow")),
        P(("wide", "narrow")),
    )
    paired = mesh.shape["narrow"] == 2 and mesh.shape["wide"] % 2 == 0
    fits = paired and mesh.shape["wide"] > 2 * REACH and REACH == 2
    return jax.shard_map(
        by_kernel if fits else by_collectives,
        mesh=mesh,
        in_specs=placed,
        out_specs=P(None, "narrow", "wide"),
        check_vma=False,
    )
```

```python
import functools

import jax
import jax.numpy as jnp
from jax import lax
from jax.experimental import pallas as pl
from jax.experimental.pallas import tpu as pltpu
from jax.sharding import PartitionSpec as P

DENOM = 256
REACH = 2
TB_DEV = 64


wet_limit = 0.001


def passed_along(block, axis, distance):
    devices = range(lax.axis_size(axis))
    route = [((i - distance) % len(devices), i) for i in devices]
    return lax.ppermute(block, axis, route)


def unpack_counts(packed_words):
    return jnp.concatenate([packed_words % 65536, packed_words // 65536], axis=-2)


def block_sums(targets, received, block_count):
    owners = jnp.arange(block_count, dtype=jnp.int32)
    select = (targets[:, None] == owners[None, :]).astype(jnp.bfloat16)
    return jnp.einsum("rq,rlcb->lcqb", select, received, preferred_element_type=jnp.float32)


def by_collectives(src_field, src_depth, packed_counts, pair_source, pair_home, pair_count):
    narrow_size = lax.axis_size("narrow")
    wide_size = lax.axis_size("wide")
    field_vars = src_field.shape[0]
    components = field_vars + 1
    block_cells = packed_counts.shape[2]
    own_cells = src_depth.shape[0]
    own_tiles = own_cells // block_cells
    pair_slots = pair_source.shape[0]
    offset_count = 2 * REACH + 1
    capacity = max(2, 2 * pair_slots // offset_count)
    own_field = lax.all_to_all(src_field, "narrow", split_axis=2, concat_axis=1, tiled=True)
    levels = own_field.shape[1]
    part_levels = levels // narrow_size
    level_ids = jnp.arange(levels, dtype=jnp.int32)
    wet_levels = level_ids[:, None] < src_depth[None, :]
    masked = jnp.where(wet_levels[None, :, :], own_field, jnp.zeros_like(own_field))
    stacked = jnp.concatenate(
        [jnp.transpose(masked, (1, 0, 2)), wet_levels.astype(jnp.bfloat16)[:, None, :]], axis=1
    )
    by_tile = jnp.transpose(stacked.reshape(levels * components, own_tiles, block_cells), (1, 0, 2))
    picked = jnp.take(by_tile, pair_source, axis=0)
    weight = (unpack_counts(packed_counts).astype(jnp.float32) / DENOM).astype(jnp.bfloat16)
    pair_terms = lax.dot_general(
        picked, weight, (((2,), (2,)), ((0,), (0,))), preferred_element_type=jnp.float32
    )
    pair_terms = pair_terms.astype(jnp.bfloat16)
    is_live = jnp.arange(pair_slots, dtype=jnp.int32) < pair_count[0]
    wide_index = lax.axis_index("wide")
    destination = pair_home // TB_DEV
    local_block = pair_home % TB_DEV
    offset_index = (destination - wide_index + REACH + wide_size) % wide_size
    bound_for = (
        (offset_index[:, None] == jnp.arange(offset_count, dtype=jnp.int32)[None, :])
        & is_live[:, None]
    ).astype(jnp.int32)
    before = jnp.cumsum(bound_for, axis=0) - bound_for
    position = jnp.sum(before * bound_for, axis=1)
    slot_index = jnp.where(is_live, offset_index * capacity + position, offset_count * capacity)
    outgoing = (
        jnp.zeros((offset_count * capacity, levels * components, block_cells), jnp.bfloat16)
        .at[slot_index]
        .set(pair_terms, mode="drop")
    )
    targets = (
        jnp.full((offset_count * capacity,), TB_DEV, jnp.int32)
        .at[slot_index]
        .set(local_block, mode="drop")
    )
    outgoing = outgoing.reshape(offset_count, capacity, levels, components, block_cells)
    targets = targets.reshape(offset_count, capacity)
    shift_list = [shift_by for shift_by in range(-REACH, REACH + 1) if shift_by != 0]
    partial_value = block_sums(targets[REACH], outgoing[REACH], TB_DEV)
    for shift_by in shift_list:
        moved_terms, moved_owners = passed_along(
            (outgoing[REACH + shift_by], targets[REACH + shift_by]), "wide", shift_by
        )
        partial_value = partial_value + block_sums(moved_owners, moved_terms, TB_DEV)
    block_totals = lax.psum_scatter(partial_value, "narrow", scatter_dimension=0, tiled=True)
    numerators = block_totals[:, :field_vars]
    wet_total = block_totals[:, field_vars]
    covered = wet_total > wet_limit
    safe_wet = jnp.where(covered, wet_total, jnp.ones_like(wet_total))
    result = jnp.where(covered[:, None], numerators / safe_wet[:, None], jnp.zeros_like(numerators))
    result = jnp.transpose(result, (1, 0, 2, 3)).reshape(
        field_vars, part_levels, TB_DEV * block_cells
    )
    return result.astype(jnp.bfloat16)


SELF, MATE, RELAY, AHEAD, BEHIND = range(5)
LOADS = 8
BATCHES = 4
EARLY = 3
UNROLL = 16
SKEW = 8


def remap_kernel(
    sizes,
    field_hbm,
    depth_hbm,
    packed_hbm,
    source_hbm,
    home_hbm,
    count_hbm,
    out_ref,
    field,
    depth,
    source,
    home,
    count,
    field_in,
    slot_own,
    slot_in,
    words,
    weight,
    stacked,
    terms,
    cross_out,
    cross_in,
    own_terms,
    self_sum,
    sums_out,
    mate_in,
    ahead_in,
    behind_in,
    load_sems,
    small_sems,
    entry_sems,
    early_sems,
    cross_sems,
    mate_sems,
    ahead_sems,
    behind_sems,
):
    wide_size, fields, levels, tiles, cells, pairs = sizes
    components = fields + 1
    rows = components * levels
    pitch = pairs + SKEW
    w = lax.axis_index("wide")
    n = lax.axis_index("narrow")
    other = 1 - n
    sign = 1 - 2 * lax.rem(w, 2)
    mate = w + sign
    ahead = lax.rem(w + 2 * sign + wide_size, wide_size)
    behind = lax.rem(w - 2 * sign + wide_size, wide_size)

    barrier = pltpu.get_barrier_semaphore()
    for place in ((w, other), (mate, n), (ahead, n), (behind, n)):
        pl.semaphore_signal(
            barrier, inc=1, device_id=place, device_id_type=pl.DeviceIdType.MESH
        )

    small = []
    for i, (src, dst) in enumerate(
        (
            (field_hbm, field),
            (home_hbm, home),
            (count_hbm, count),
            (depth_hbm, depth),
            (source_hbm, source),
        )
    ):
        load = pltpu.make_async_copy(src, dst, small_sems.at[i])
        load.start()
        small.append(load)
    per_load = pairs // LOADS
    loads = []
    for i in range(LOADS):
        span = pl.ds(i * per_load, per_load)
        load = pltpu.make_async_copy(packed_hbm.at[span], words.at[span], load_sems.at[i])
        load.start()
        loads.append(load)

    def remote(src, dst, sems, index, place):
        return pltpu.make_async_remote_copy(
            src_ref=src,
            dst_ref=dst,
            send_sem=sems.at[(0,) + index],
            recv_sem=sems.at[(1,) + index],
            device_id=place,
            device_id_type=pl.DeviceIdType.MESH,
        )

    small[0].wait()
    small[1].wait()
    small[2].wait()
    wide_home = lax.div(home[...], TB_DEV)
    offset = lax.rem(wide_home - w + REACH + wide_size, wide_size) - REACH
    toward = offset * sign
    slot = jnp.where(toward > 0, 2 * toward - 1, -2 * toward)
    is_live = lax.broadcasted_iota(jnp.int32, (1, pairs), 1) < count[0]
    slot_own[...] = jnp.where(is_live, slot * TB_DEV + home[...] - wide_home * TB_DEV, -1)

    pl.semaphore_wait(barrier, 4)
    own_cells = tiles * cells
    entry = [
        remote(
            field.at[:, :, pl.ds(pl.multiple_of(other * own_cells, own_cells), own_cells)],
            field_in,
            entry_sems,
            (0,),
            (w, other),
        ),
        remote(slot_own, slot_in, entry_sems, (1,), (w, other)),
    ]
    for copy in entry:
        copy.start()

    level_ids = lax.broadcasted_iota(jnp.int32, (levels, cells), 0)

    def stack(side, group, read):
        for tile in range(tiles):
            wet = level_ids + group * levels < depth[pl.ds(tile, 1), :]
            for k in range(components):
                value = read(k, tile).astype(jnp.float32) if k < fields else 1.0
                stacked[tile, pl.ds(side * rows + k * levels, levels), :] = jnp.where(
                    wet, value, 0.0
                )

    small[3].wait()
    small[4].wait()
    own_start = n * own_cells
    stack(
        1,
        n,
        lambda k, tile: field[k, :, pl.ds(pl.multiple_of(own_start + tile * cells, cells), cells)],
    )

    half = cells // 2
    for i in range(LOADS):
        loads[i].wait()

        def unpack(step, carry):
            for u in range(UNROLL):
                p = i * per_load + step * UNROLL + u
                word = words[p]
                low = (word & 65535).astype(jnp.float32).astype(jnp.bfloat16)
                high = (word >> 16).astype(jnp.float32).astype(jnp.bfloat16)
                weight[p, pl.ds(0, half), :] = low
                weight[p, pl.ds(half, half), :] = high
            return carry

        lax.fori_loop(0, per_load // UNROLL, unpack, 0)

    entry[0].wait()
    stack(0, other, lambda k, tile: field_in[k, :, pl.ds(tile * cells, cells)])

    per_batch = pairs // BATCHES

    def rounded(side, level, k, start, count):
        row = side * rows + k * levels + level
        return terms[pl.ds(row * pitch + start, count), :].astype(jnp.bfloat16)

    cross = []
    for batch in range(BATCHES):
        first = batch * per_batch

        def multiply(step, carry):
            for u in range(UNROLL):
                p = first + step * UNROLL + u
                values = stacked[source[p]].astype(jnp.bfloat16)
                term = lax.dot_general(
                    values, weight[p], (((1,), (1,)), ((), ())),
                    preferred_element_type=jnp.float32,
                )
                terms[pl.ds(p, 2 * rows, stride=pitch), :] = term * (1.0 / DENOM)
            return carry

        lax.fori_loop(0, per_batch // UNROLL, multiply, 0)
        span = pl.ds(first, per_batch)
        for level in range(EARLY):
            for k in range(components):
                cross_out[level, k, span, :] = rounded(0, level, k, first, per_batch)
            copy = remote(
                cross_out.at[level, :, span, :],
                cross_in.at[level, :, span, :],
                early_sems,
                (level, batch),
                (w, other),
            )
            copy.start()
            cross.append((level, copy))
    for level in range(EARLY, levels):
        for k in range(components):
            cross_out[level, k] = rounded(0, level, k, 0, pairs)
        copy = remote(
            cross_out.at[level], cross_in.at[level], cross_sems, (level - EARLY,), (w, other)
        )
        copy.start()
        cross.append((level, copy))
    for level in range(levels):
        for k in range(components):
            own_terms[level, k] = rounded(1, level, k, 0, pairs)

    entry[1].wait()
    slots = lax.broadcasted_iota(jnp.int32, (5 * TB_DEV, pairs), 0)
    select = jnp.concatenate(
        [
            jnp.where(slots == slot_own[...], 1.0, 0.0).astype(jnp.bfloat16),
            jnp.where(slots == slot_in[...], 1.0, 0.0).astype(jnp.bfloat16),
        ],
        axis=1,
    )

    to_mate, to_ahead, to_behind = [], [], []

    def pass_on(level):
        to_mate[level].wait_recv()
        for k in range(components):
            sums_out[level, AHEAD - 1, k] = (
                sums_out[level, AHEAD - 1, k].astype(jnp.float32)
                + mate_in[level, RELAY - 1, k].astype(jnp.float32)
            ).astype(jnp.bfloat16)
        copy = remote(
            sums_out.at[level, AHEAD - 1], ahead_in.at[level], ahead_sems, (level,), (ahead, n)
        )
        copy.start()
        to_ahead.append(copy)

    for level in range(levels):
        for of_level, copy in cross:
            if of_level == level:
                copy.wait_recv()
        for k in range(components):
            pair_values = jnp.concatenate([own_terms[level, k], cross_in[level, k]], axis=0)
            sums = jnp.dot(select, pair_values, preferred_element_type=jnp.float32)
            self_sum[level, k] = sums[:TB_DEV]
            for slot in (MATE, RELAY, AHEAD, BEHIND):
                sums_out[level, slot - 1, k] = sums[
                    slot * TB_DEV : (slot + 1) * TB_DEV
                ].astype(jnp.bfloat16)
        copy = remote(
            sums_out.at[level, pl.ds(0, 2)], mate_in.at[level], mate_sems, (level,), (mate, n)
        )
        copy.start()
        to_mate.append(copy)
        copy = remote(
            sums_out.at[level, BEHIND - 1], behind_in.at[level], behind_sems, (level,), (behind, n)
        )
        copy.start()
        to_behind.append(copy)
        if level > 0:
            pass_on(level - 1)
    pass_on(levels - 1)

    for level in range(levels):
        to_behind[level].wait_recv()
        to_ahead[level].wait_recv()

        def total(k):
            return (
                self_sum[level, k]
                + mate_in[level, MATE - 1, k].astype(jnp.float32)
                + ahead_in[level, k].astype(jnp.float32)
                + behind_in[level, k].astype(jnp.float32)
            )

        wet_total = total(fields)
        covered = wet_total > wet_limit
        safe_wet = jnp.where(covered, wet_total, 1.0)
        for k in range(fields):
            out_ref[k, level] = jnp.where(covered, total(k) / safe_wet, 0.0).astype(out_ref.dtype)
    for _, copy in cross:
        copy.wait_send()
    for copy in to_mate + to_ahead + to_behind:
        copy.wait_send()


def by_kernel(src_field, src_depth, packed_counts, pair_source, pair_home, pair_count):
    wide_size = lax.axis_size("wide")
    fields, levels, _ = src_field.shape
    pairs, _, cells = packed_counts.shape
    tiles = src_depth.shape[0] // cells
    components = fields + 1
    rows = components * levels
    sizes = (wide_size, fields, levels, tiles, cells, pairs)
    hbm = pl.BlockSpec(memory_space=pltpu.HBM)
    bf16, f32, i32 = jnp.bfloat16, jnp.float32, jnp.int32
    terms_shape = (levels, components, pairs, cells)
    sums_shape = (components, TB_DEV, cells)
    copies = pltpu.SemaphoreType.DMA((2, levels))
    result = pl.pallas_call(
        functools.partial(remap_kernel, sizes),
        out_shape=jax.ShapeDtypeStruct((fields, levels, TB_DEV, cells), bf16),
        in_specs=[hbm] * 6,
        out_specs=pl.BlockSpec(memory_space=pltpu.VMEM),
        scratch_shapes=[
            pltpu.VMEM(src_field.shape, bf16),
            pltpu.VMEM((tiles, cells), i32),
            pltpu.SMEM((pairs,), i32),
            pltpu.VMEM((1, pairs), i32),
            pltpu.SMEM((1,), i32),
            pltpu.VMEM((fields, levels, tiles * cells), bf16),
            pltpu.VMEM((1, pairs), i32),
            pltpu.VMEM((1, pairs), i32),
            pltpu.VMEM((pairs, cells // 2, cells), i32),
            pltpu.VMEM((pairs, cells, cells), bf16),
            pltpu.VMEM((tiles, 2 * rows, cells), f32),
            pltpu.VMEM((2 * rows * (pairs + SKEW), cells), f32),
            pltpu.VMEM(terms_shape, bf16),
            pltpu.VMEM(terms_shape, bf16),
            pltpu.VMEM(terms_shape, bf16),
            pltpu.VMEM((levels,) + sums_shape, f32),
            pltpu.VMEM((levels, 4) + sums_shape, bf16),
            pltpu.VMEM((levels, 2) + sums_shape, bf16),
            pltpu.VMEM((levels,) + sums_shape, bf16),
            pltpu.VMEM((levels,) + sums_shape, bf16),
            pltpu.SemaphoreType.DMA((LOADS,)),
            pltpu.SemaphoreType.DMA((5,)),
            pltpu.SemaphoreType.DMA((2, 2)),
            pltpu.SemaphoreType.DMA((2, EARLY, BATCHES)),
            pltpu.SemaphoreType.DMA((2, levels - EARLY)),
            copies,
            copies,
            copies,
        ],
        compiler_params=pltpu.CompilerParams(
            collective_id=0, has_side_effects=True, vmem_limit_bytes=67043328
        ),
        name="remap",
    )(
        src_field,
        src_depth.reshape(tiles, cells),
        packed_counts,
        pair_source,
        pair_home.reshape(1, pairs),
        pair_count,
    )
    return result.reshape(fields, levels, TB_DEV * cells)


def solution(mesh):
    placed = (
        P(None, "narrow", "wide"),
        P(("wide", "narrow")),
        P(("wide", "narrow"), None, None),
        P(("wide", "narrow")),
        P(("wide", "narrow")),
        P(("wide", "narrow")),
    )
    paired = mesh.shape["narrow"] == 2 and mesh.shape["wide"] % 2 == 0
    fits = paired and mesh.shape["wide"] > 2 * REACH and REACH == 2
    return jax.shard_map(
        by_kernel if fits else by_collectives,
        mesh=mesh,
        in_specs=placed,
        out_specs=P(None, "narrow", "wide"),
        check_vma=False,
    )
```

```python
import functools

import jax
import jax.numpy as jnp
from jax import lax
from jax.experimental import pallas as pl
from jax.experimental.pallas import tpu as pltpu
from jax.sharding import PartitionSpec as P

DENOM = 256
REACH = 2
TB_DEV = 64


wet_limit = 0.001


def passed_along(block, axis, distance):
    devices = range(lax.axis_size(axis))
    route = [((i - distance) % len(devices), i) for i in devices]
    return lax.ppermute(block, axis, route)


def unpack_counts(packed_words):
    return jnp.concatenate([packed_words % 65536, packed_words // 65536], axis=-2)


def block_sums(targets, received, block_count):
    owners = jnp.arange(block_count, dtype=jnp.int32)
    select = (targets[:, None] == owners[None, :]).astype(jnp.bfloat16)
    return jnp.einsum("rq,rlcb->lcqb", select, received, preferred_element_type=jnp.float32)


def by_collectives(src_field, src_depth, packed_counts, pair_source, pair_home, pair_count):
    narrow_size = lax.axis_size("narrow")
    wide_size = lax.axis_size("wide")
    field_vars = src_field.shape[0]
    components = field_vars + 1
    block_cells = packed_counts.shape[2]
    own_cells = src_depth.shape[0]
    own_tiles = own_cells // block_cells
    pair_slots = pair_source.shape[0]
    offset_count = 2 * REACH + 1
    capacity = max(2, 2 * pair_slots // offset_count)
    own_field = lax.all_to_all(src_field, "narrow", split_axis=2, concat_axis=1, tiled=True)
    levels = own_field.shape[1]
    part_levels = levels // narrow_size
    level_ids = jnp.arange(levels, dtype=jnp.int32)
    wet_levels = level_ids[:, None] < src_depth[None, :]
    masked = jnp.where(wet_levels[None, :, :], own_field, jnp.zeros_like(own_field))
    stacked = jnp.concatenate(
        [jnp.transpose(masked, (1, 0, 2)), wet_levels.astype(jnp.bfloat16)[:, None, :]], axis=1
    )
    by_tile = jnp.transpose(stacked.reshape(levels * components, own_tiles, block_cells), (1, 0, 2))
    picked = jnp.take(by_tile, pair_source, axis=0)
    weight = (unpack_counts(packed_counts).astype(jnp.float32) / DENOM).astype(jnp.bfloat16)
    pair_terms = lax.dot_general(
        picked, weight, (((2,), (2,)), ((0,), (0,))), preferred_element_type=jnp.float32
    )
    pair_terms = pair_terms.astype(jnp.bfloat16)
    is_live = jnp.arange(pair_slots, dtype=jnp.int32) < pair_count[0]
    wide_index = lax.axis_index("wide")
    destination = pair_home // TB_DEV
    local_block = pair_home % TB_DEV
    offset_index = (destination - wide_index + REACH + wide_size) % wide_size
    bound_for = (
        (offset_index[:, None] == jnp.arange(offset_count, dtype=jnp.int32)[None, :])
        & is_live[:, None]
    ).astype(jnp.int32)
    before = jnp.cumsum(bound_for, axis=0) - bound_for
    position = jnp.sum(before * bound_for, axis=1)
    slot_index = jnp.where(is_live, offset_index * capacity + position, offset_count * capacity)
    outgoing = (
        jnp.zeros((offset_count * capacity, levels * components, block_cells), jnp.bfloat16)
        .at[slot_index]
        .set(pair_terms, mode="drop")
    )
    targets = (
        jnp.full((offset_count * capacity,), TB_DEV, jnp.int32)
        .at[slot_index]
        .set(local_block, mode="drop")
    )
    outgoing = outgoing.reshape(offset_count, capacity, levels, components, block_cells)
    targets = targets.reshape(offset_count, capacity)
    shift_list = [shift_by for shift_by in range(-REACH, REACH + 1) if shift_by != 0]
    partial_value = block_sums(targets[REACH], outgoing[REACH], TB_DEV)
    for shift_by in shift_list:
        moved_terms, moved_owners = passed_along(
            (outgoing[REACH + shift_by], targets[REACH + shift_by]), "wide", shift_by
        )
        partial_value = partial_value + block_sums(moved_owners, moved_terms, TB_DEV)
    block_totals = lax.psum_scatter(partial_value, "narrow", scatter_dimension=0, tiled=True)
    numerators = block_totals[:, :field_vars]
    wet_total = block_totals[:, field_vars]
    covered = wet_total > wet_limit
    safe_wet = jnp.where(covered, wet_total, jnp.ones_like(wet_total))
    result = jnp.where(covered[:, None], numerators / safe_wet[:, None], jnp.zeros_like(numerators))
    result = jnp.transpose(result, (1, 0, 2, 3)).reshape(
        field_vars, part_levels, TB_DEV * block_cells
    )
    return result.astype(jnp.bfloat16)


SELF, MATE, RELAY, AHEAD, BEHIND = range(5)
LOADS = 8
BATCHES = 4
EARLY = 2
UNROLL = 16
SKEW = 8


def remap_kernel(
    sizes,
    field_hbm,
    depth_hbm,
    packed_hbm,
    source_hbm,
    home_hbm,
    count_hbm,
    out_ref,
    field,
    depth,
    source,
    home,
    count,
    field_in,
    slot_own,
    slot_in,
    words,
    weight,
    stacked,
    terms,
    cross_out,
    cross_in,
    own_terms,
    self_sum,
    sums_out,
    mate_in,
    ahead_in,
    behind_in,
    load_sems,
    small_sems,
    entry_sems,
    early_sems,
    cross_sems,
    mate_sems,
    ahead_sems,
    behind_sems,
):
    wide_size, fields, levels, tiles, cells, pairs = sizes
    components = fields + 1
    rows = components * levels
    pitch = pairs + SKEW
    w = lax.axis_index("wide")
    n = lax.axis_index("narrow")
    other = 1 - n
    sign = 1 - 2 * lax.rem(w, 2)
    mate = w + sign
    ahead = lax.rem(w + 2 * sign + wide_size, wide_size)
    behind = lax.rem(w - 2 * sign + wide_size, wide_size)

    barrier = pltpu.get_barrier_semaphore()
    for place in ((w, other), (mate, n), (ahead, n), (behind, n)):
        pl.semaphore_signal(
            barrier, inc=1, device_id=place, device_id_type=pl.DeviceIdType.MESH
        )

    small = []
    for i, (src, dst) in enumerate(
        (
            (field_hbm, field),
            (home_hbm, home),
            (count_hbm, count),
            (depth_hbm, depth),
            (source_hbm, source),
        )
    ):
        load = pltpu.make_async_copy(src, dst, small_sems.at[i])
        load.start()
        small.append(load)
    per_load = pairs // LOADS
    loads = []
    for i in range(LOADS):
        span = pl.ds(i * per_load, per_load)
        load = pltpu.make_async_copy(packed_hbm.at[span], words.at[span], load_sems.at[i])
        load.start()
        loads.append(load)

    def remote(src, dst, sems, index, place):
        return pltpu.make_async_remote_copy(
            src_ref=src,
            dst_ref=dst,
            send_sem=sems.at[(0,) + index],
            recv_sem=sems.at[(1,) + index],
            device_id=place,
            device_id_type=pl.DeviceIdType.MESH,
        )

    own_cells = tiles * cells
    theirs = pl.ds(pl.multiple_of(other * own_cells, own_cells), own_cells)
    small[0].wait()
    pl.semaphore_wait(barrier, 4)
    entry = [remote(field.at[:, :, theirs], field_in, entry_sems, (0,), (w, other))]
    entry[0].start()

    small[1].wait()
    small[2].wait()
    wide_home = lax.div(home[...], TB_DEV)
    offset = lax.rem(wide_home - w + REACH + wide_size, wide_size) - REACH
    toward = offset * sign
    slot = jnp.where(toward > 0, 2 * toward - 1, -2 * toward)
    is_live = lax.broadcasted_iota(jnp.int32, (1, pairs), 1) < count[0]
    slot_own[...] = jnp.where(is_live, slot * TB_DEV + home[...] - wide_home * TB_DEV, -1)
    entry.append(remote(slot_own, slot_in, entry_sems, (1,), (w, other)))
    entry[1].start()

    level_ids = lax.broadcasted_iota(jnp.int32, (levels, cells), 0)

    def stack(side, group, read):
        for tile in range(tiles):
            wet = level_ids + group * levels < depth[pl.ds(tile, 1), :]
            for k in range(components):
                value = read(k, tile).astype(jnp.float32) if k < fields else 1.0
                stacked[tile, pl.ds(side * rows + k * levels, levels), :] = jnp.where(
                    wet, value, 0.0
                )

    small[3].wait()
    small[4].wait()
    own_start = n * own_cells
    stack(
        1,
        n,
        lambda k, tile: field[k, :, pl.ds(pl.multiple_of(own_start + tile * cells, cells), cells)],
    )

    half = cells // 2
    for i in range(LOADS):
        loads[i].wait()

        def unpack(step, carry):
            for u in range(UNROLL):
                p = i * per_load + step * UNROLL + u
                word = words[p]
                low = (word & 65535).astype(jnp.float32).astype(jnp.bfloat16)
                high = (word >> 16).astype(jnp.float32).astype(jnp.bfloat16)
                weight[p, pl.ds(0, half), :] = low
                weight[p, pl.ds(half, half), :] = high
            return carry

        lax.fori_loop(0, per_load // UNROLL, unpack, 0)

    per_batch = pairs // BATCHES

    def multiply(side, first, count):
        def body(step, carry):
            for u in range(UNROLL):
                p = first + step * UNROLL + u
                values = stacked[source[p], pl.ds(side * rows, rows), :].astype(jnp.bfloat16)
                term = lax.dot_general(
                    values, weight[p], (((1,), (1,)), ((), ())),
                    preferred_element_type=jnp.float32,
                )
                terms[pl.ds(side * rows * pitch + p, rows, stride=pitch), :] = term * (1.0 / DENOM)
            return carry

        lax.fori_loop(0, count // UNROLL, body, 0)

    def rounded(side, level, k, start, count):
        row = side * rows + k * levels + level
        return terms[pl.ds(row * pitch + start, count), :].astype(jnp.bfloat16)

    entry[0].wait()
    stack(0, other, lambda k, tile: field_in[k, :, pl.ds(tile * cells, cells)])

    cross = []
    for batch in range(BATCHES):
        first = batch * per_batch
        multiply(0, first, per_batch)
        span = pl.ds(first, per_batch)
        for level in range(EARLY):
            for k in range(components):
                cross_out[level, k, span, :] = rounded(0, level, k, first, per_batch)
            copy = remote(
                cross_out.at[level, :, span, :],
                cross_in.at[level, :, span, :],
                early_sems,
                (level, batch),
                (w, other),
            )
            copy.start()
            cross.append((level, copy))
    for level in range(EARLY, levels):
        for k in range(components):
            cross_out[level, k] = rounded(0, level, k, 0, pairs)
        copy = remote(
            cross_out.at[level], cross_in.at[level], cross_sems, (level - EARLY,), (w, other)
        )
        copy.start()
        cross.append((level, copy))

    multiply(1, 0, pairs)
    for level in range(levels):
        for k in range(components):
            own_terms[level, k] = rounded(1, level, k, 0, pairs)

    entry[1].wait()
    slots = lax.broadcasted_iota(jnp.int32, (5 * TB_DEV, pairs), 0)
    select = jnp.concatenate(
        [
            jnp.where(slots == slot_own[...], 1.0, 0.0).astype(jnp.bfloat16),
            jnp.where(slots == slot_in[...], 1.0, 0.0).astype(jnp.bfloat16),
        ],
        axis=1,
    )

    to_mate, to_ahead, to_behind = [], [], []

    def pass_on(level):
        to_mate[level].wait_recv()
        for k in range(components):
            sums_out[level, AHEAD - 1, k] = (
                sums_out[level, AHEAD - 1, k].astype(jnp.float32)
                + mate_in[level, RELAY - 1, k].astype(jnp.float32)
            ).astype(jnp.bfloat16)
        copy = remote(
            sums_out.at[level, AHEAD - 1], ahead_in.at[level], ahead_sems, (level,), (ahead, n)
        )
        copy.start()
        to_ahead.append(copy)

    for level in range(levels):
        for of_level, copy in cross:
            if of_level == level:
                copy.wait_recv()
        for k in range(components):
            pair_values = jnp.concatenate([own_terms[level, k], cross_in[level, k]], axis=0)
            sums = jnp.dot(select, pair_values, preferred_element_type=jnp.float32)
            self_sum[level, k] = sums[:TB_DEV]
            for slot in (MATE, RELAY, AHEAD, BEHIND):
                sums_out[level, slot - 1, k] = sums[
                    slot * TB_DEV : (slot + 1) * TB_DEV
                ].astype(jnp.bfloat16)
        copy = remote(
            sums_out.at[level, pl.ds(0, 2)], mate_in.at[level], mate_sems, (level,), (mate, n)
        )
        copy.start()
        to_mate.append(copy)
        copy = remote(
            sums_out.at[level, BEHIND - 1], behind_in.at[level], behind_sems, (level,), (behind, n)
        )
        copy.start()
        to_behind.append(copy)
        if level > 0:
            pass_on(level - 1)
    pass_on(levels - 1)

    for level in range(levels):
        to_behind[level].wait_recv()
        to_ahead[level].wait_recv()

        def total(k):
            return (
                self_sum[level, k]
                + mate_in[level, MATE - 1, k].astype(jnp.float32)
                + ahead_in[level, k].astype(jnp.float32)
                + behind_in[level, k].astype(jnp.float32)
            )

        wet_total = total(fields)
        covered = wet_total > wet_limit
        safe_wet = jnp.where(covered, wet_total, 1.0)
        for k in range(fields):
            out_ref[k, level] = jnp.where(covered, total(k) / safe_wet, 0.0).astype(out_ref.dtype)
    for _, copy in cross:
        copy.wait_send()
    for copy in to_mate + to_ahead + to_behind:
        copy.wait_send()


def by_kernel(src_field, src_depth, packed_counts, pair_source, pair_home, pair_count):
    wide_size = lax.axis_size("wide")
    fields, levels, _ = src_field.shape
    pairs, _, cells = packed_counts.shape
    tiles = src_depth.shape[0] // cells
    components = fields + 1
    rows = components * levels
    sizes = (wide_size, fields, levels, tiles, cells, pairs)
    hbm = pl.BlockSpec(memory_space=pltpu.HBM)
    bf16, f32, i32 = jnp.bfloat16, jnp.float32, jnp.int32
    terms_shape = (levels, components, pairs, cells)
    sums_shape = (components, TB_DEV, cells)
    copies = pltpu.SemaphoreType.DMA((2, levels))
    result = pl.pallas_call(
        functools.partial(remap_kernel, sizes),
        out_shape=jax.ShapeDtypeStruct((fields, levels, TB_DEV, cells), bf16),
        in_specs=[hbm] * 6,
        out_specs=pl.BlockSpec(memory_space=pltpu.VMEM),
        scratch_shapes=[
            pltpu.VMEM(src_field.shape, bf16),
            pltpu.VMEM((tiles, cells), i32),
            pltpu.SMEM((pairs,), i32),
            pltpu.VMEM((1, pairs), i32),
            pltpu.SMEM((1,), i32),
            pltpu.VMEM((fields, levels, tiles * cells), bf16),
            pltpu.VMEM((1, pairs), i32),
            pltpu.VMEM((1, pairs), i32),
            pltpu.VMEM((pairs, cells // 2, cells), i32),
            pltpu.VMEM((pairs, cells, cells), bf16),
            pltpu.VMEM((tiles, 2 * rows, cells), f32),
            pltpu.VMEM((2 * rows * (pairs + SKEW), cells), f32),
            pltpu.VMEM(terms_shape, bf16),
            pltpu.VMEM(terms_shape, bf16),
            pltpu.VMEM(terms_shape, bf16),
            pltpu.VMEM((levels,) + sums_shape, f32),
            pltpu.VMEM((levels, 4) + sums_shape, bf16),
            pltpu.VMEM((levels, 2) + sums_shape, bf16),
            pltpu.VMEM((levels,) + sums_shape, bf16),
            pltpu.VMEM((levels,) + sums_shape, bf16),
            pltpu.SemaphoreType.DMA((LOADS,)),
            pltpu.SemaphoreType.DMA((5,)),
            pltpu.SemaphoreType.DMA((2, 2)),
            pltpu.SemaphoreType.DMA((2, EARLY, BATCHES)),
            pltpu.SemaphoreType.DMA((2, levels - EARLY)),
            copies,
            copies,
            copies,
        ],
        compiler_params=pltpu.CompilerParams(
            collective_id=0, has_side_effects=True, vmem_limit_bytes=67043328
        ),
        name="remap",
    )(
        src_field,
        src_depth.reshape(tiles, cells),
        packed_counts,
        pair_source,
        pair_home.reshape(1, pairs),
        pair_count,
    )
    return result.reshape(fields, levels, TB_DEV * cells)


def solution(mesh):
    placed = (
        P(None, "narrow", "wide"),
        P(("wide", "narrow")),
        P(("wide", "narrow"), None, None),
        P(("wide", "narrow")),
        P(("wide", "narrow")),
        P(("wide", "narrow")),
    )
    paired = mesh.shape["narrow"] == 2 and mesh.shape["wide"] % 2 == 0
    fits = paired and mesh.shape["wide"] > 2 * REACH and REACH == 2
    return jax.shard_map(
        by_kernel if fits else by_collectives,
        mesh=mesh,
        in_specs=placed,
        out_specs=P(None, "narrow", "wide"),
        check_vma=False,
    )
```
